32 devices in a mesh: gx: 4 (over x, core), gy: 4 (over z), gz: 2 (over y).
Axes of the slice: x: 2, y: 2, z: 4, core: 2. Of those that a mesh axis runs over, the one named last changes fastest.
Arguments:
- amplitudes: bfloat16 [2, 16384, 2048], P(None, ('gx', 'gy', 'gz')), may hold values from -6 to 6
- pauli_x: int32 [200], replicated, may hold values from 0 to 2047, as said below
- pauli_z: int32 [200], replicated, may hold values from 0 to 2047
- pauli_phase: int32 [200], replicated, may hold values from 0 to 3
Outputs:
- density_real: float32 [2048, 2048], P(('gx', 'gy', 'gz'))
- density_imag: float32 [2048, 2048], P(('gx', 'gy', 'gz'))
- expectations: float32 [2, 200], replicated
The draws below stay inside these ranges and needn't reach their ends.
Inputs may be any that keep to these rules, and one draw needn't show every extreme that they name: Bit q of the mask acts on kept qubit q (the bit of weight 2^q of the last index); pauli_x and pauli_z of a term are never both zero.
All inputs are finite; a program needn't handle non-finite values.
Results may differ from the reference program's by a relative error of at most 0.0003.
Values sent between devices are 32-bit elements; how exact they have to be, the bound alone decides.
A program may use at most 192 MiB of HBM per device.

```python
import jax
import jax.numpy as jnp
from jax import lax

QUBITS = 11
R = 2048
COLS_ALL = 16384
TERMS = 200


def pauli_masks(key):
    flips = jax.random.randint(jax.random.fold_in(key, 11), (TERMS,), 0, R).astype(jnp.int32)
    phases = jax.random.randint(jax.random.fold_in(key, 23), (TERMS,), 0, R).astype(jnp.int32)
    both_zero = jnp.logical_and(flips == 0, phases == 0)
    phases = jnp.where(both_zero, jnp.int32(1), phases)
    return (flips, phases)


def draw_pauli_x(key, part):
    return pauli_masks(key)[0]


def draw_pauli_z(key, part):
    return pauli_masks(key)[1]


def with_ends(result, key, low, top_value):
    shape = result.shape
    index_at = [jax.random.randint(jax.random.fold_in(key, axis), (), 0, shape[axis]) for axis in range(len(shape))]
    result = result.at[tuple(index_at)].set(low)
    longest = shape.index(max(shape))
    index_at[longest] = (index_at[longest] + 1) % shape[longest]
    return result.at[tuple(index_at)].set(top_value)


def shard_levels(key, extent, cuts, low, high):
    gain, own = 1.0, jax.random.fold_in(key, 6)
    for position, parts in cuts:
        heights = jnp.exp(jax.random.uniform(jax.random.fold_in(own, position), (parts,), jnp.float32, low / len(cuts), high / len(cuts)))
        gain = gain * jnp.repeat(heights, extent[position] // parts).reshape([-1 if axis == position else 1 for axis in range(len(extent))])
    return gain


def bell_draw(stream_key, extent, width, limit, shards=(), kind=jnp.bfloat16):
    array = width * jax.random.normal(stream_key, extent, jnp.float32)
    if shards:
        array = array * shard_levels(stream_key, extent, shards, -0.22, 0.18)
    return jnp.clip(array, -limit, limit).astype(kind)


def setup_inputs(seed: int = 0) -> dict:
    streams_of = jax.random.split(jax.random.key(seed), 5)
    return {
        "amplitudes": bell_draw(streams_of[0], (2, COLS_ALL, R), 1.0, 6.0, ((1, 32),)),
        "pauli_x": draw_pauli_x(jax.random.fold_in(streams_of[4], 71), 0),
        "pauli_z": draw_pauli_z(jax.random.fold_in(streams_of[4], 71), 0),
        "pauli_phase": with_ends(jax.random.randint(streams_of[3], (TERMS,), 0, 4), jax.random.fold_in(streams_of[3], 1), 0, 3).astype(jnp.int32),
    }


def parity_sign(values, masks):
    anded = jnp.bitwise_and(values, masks)
    counted = jnp.zeros_like(anded)
    for bit_index in range(QUBITS):
        counted = counted + jnp.bitwise_and(jnp.right_shift(anded, bit_index), 1)
    return (1 - 2 * jnp.bitwise_and(counted, 1)).astype(jnp.float32)


def phase_parts(pauli_phase):
    phase_real = jnp.where(pauli_phase == 0, 1.0, jnp.where(pauli_phase == 2, -1.0, 0.0)).astype(jnp.float32)
    phase_imag = jnp.where(pauli_phase == 1, 1.0, jnp.where(pauli_phase == 3, -1.0, 0.0)).astype(jnp.float32)
    return phase_real, phase_imag


def reference(amplitudes, pauli_x, pauli_z, pauli_phase):
    real_part = amplitudes[0].astype(jnp.float32)
    imag_part = amplitudes[1].astype(jnp.float32)
    dims = (((0,), (0,)), ((), ()))
    high = lax.Precision.HIGHEST
    gram_real = lax.dot_general(real_part, real_part, dims, precision=high) + lax.dot_general(imag_part, imag_part, dims, precision=high)
    gram_imag = lax.dot_general(imag_part, real_part, dims, precision=high) - lax.dot_general(real_part, imag_part, dims, precision=high)
    total_cols = amplitudes.shape[1]
    density_real = gram_real / total_cols
    density_imag = gram_imag / total_cols
    row_ids = jnp.arange(R, dtype=jnp.int32)[None, :]
    partner = jnp.bitwise_xor(row_ids, pauli_x[:, None])
    picked_real = jnp.take_along_axis(density_real, partner.T, axis=1).T
    picked_imag = jnp.take_along_axis(density_imag, partner.T, axis=1).T
    signs = parity_sign(row_ids, pauli_z[:, None])
    phase_real, phase_imag = phase_parts(pauli_phase)
    sum_real = jnp.sum(signs * picked_real, axis=1)
    sum_imag = jnp.sum(signs * picked_imag, axis=1)
    expect_real = phase_real * sum_real - phase_imag * sum_imag
    expect_imag = phase_real * sum_imag + phase_imag * sum_real
    return density_real, density_imag, jnp.stack([expect_real, expect_imag], 0)
```

```python
import functools

import jax
import jax.numpy as jnp
from jax import lax
from jax.experimental import pallas as pl
from jax.experimental.pallas import tpu as pltpu
from jax.sharding import PartitionSpec as P

AXES = ("gx", "gy", "gz")
LANES = 128
MESH = pl.DeviceIdType.MESH


def log2(value):
    return value.bit_length() - 1


def flat_index(sizes):
    return (lax.axis_index("gx") * sizes[1] + lax.axis_index("gy")) * sizes[2] + lax.axis_index("gz")


def coords(flat, sizes):
    return (flat // (sizes[1] * sizes[2]), (flat // sizes[2]) % sizes[1], flat % sizes[2])


def flip(bit, by):
    return bit + by - 2 * bit * by


def stage_order(sizes):
    zs = log2(sizes[2])
    ys = log2(sizes[1])
    xs = log2(sizes[0])
    low = [zs + ys]
    rest_x = [zs + ys + t for t in range(xs - 1, 0, -1)]
    rest_z = list(range(zs - 1, -1, -1))
    rest_y = [zs + t for t in range(ys - 1, -1, -1)]
    return low + rest_x + rest_z + rest_y


def gram_kernel(sizes, total_cols, amp, kept, mirrored, ext, part, land, turned, came, load_sem, send_sem, recv_sem, msend, mrecv):
    n = sizes[0] * sizes[1] * sizes[2]
    nbits = log2(n)
    depth = amp.shape[1]
    order = amp.shape[2]
    own = order // n
    block = max(own, LANES)
    q = block // own
    blocks = order // block
    width = (blocks // 2 + 1) * block
    me = flat_index(sizes)
    bits = [(me // (1 << p)) % 2 for p in range(nbits)]
    stages = stage_order(sizes)
    half = bits[stages[0]]

    def loads():
        out = []
        for part_index in range(2):
            rows = pl.ds(part_index * depth, depth)
            out.append(pltpu.make_async_copy(amp.at[part_index], ext.at[rows, pl.ds(0, order)], load_sem.at[2 * part_index]))
            out.append(
                pltpu.make_async_copy(
                    amp.at[part_index, :, pl.ds(0, width - block)],
                    ext.at[rows, pl.ds(order, width - block)],
                    load_sem.at[2 * part_index + 1],
                )
            )
        return out

    for copy in loads():
        copy.start()

    def flips_of(v):
        by_stage = [(v >> (nbits - 1 - s)) & 1 for s in range(nbits)]
        flips = [0] * nbits
        for s, p in enumerate(stages):
            flips[p] = by_stage[s]
        if by_stage[1] != by_stage[2]:
            first, second = stages[1], stages[2]
            flips[first] = by_stage[1] * (1 - half) + by_stage[2] * half
            flips[second] = by_stage[2] * (1 - half) + by_stage[1] * half
        return flips

    def place(flips):
        return sum((1 << p) * flip(bits[p], flips[p]) for p in range(nbits))

    def name(flips):
        return sum((1 << p) * flips[p] for p in range(nbits))

    def message(where, ident, target):
        return pltpu.make_async_remote_copy(
            src_ref=part.at[where],
            dst_ref=land.at[ident],
            send_sem=send_sem.at[ident],
            recv_sem=recv_sem.at[ident],
            device_id=coords(target, sizes),
            device_id_type=MESH,
        )

    partner = [place(flips_of(1 << (nbits - 1 - s))) for s in range(nbits)]
    lowbits = log2(q)
    high = [p for p in stages[1:] if p >= lowbits]

    def row_block(u):
        flips = [0] * nbits
        flips[stages[0]] = 1 - u % 2
        for j, p in enumerate(high):
            flips[p] = 1 - (u // (1 << (len(high) - j))) % 2
        return flips

    for copy in loads():
        copy.wait()

    def compute(u, _):
        @pl.when(u % 2 == 1)
        def _():
            for g in range(q):
                flips = row_block(u - 1)
                for p in range(lowbits):
                    flips[p] = (g >> p) & 1
                message(place(flips), name(flips), partner[0]).start()

        flips = row_block(u)
        first = sum((1 << p) * flip(bits[p], flips[p]) for p in range(lowbits, nbits))
        start = pl.multiple_of(first * own, block)
        lhs = ext[:, pl.ds(start, block)]
        crossed = jnp.concatenate([lhs[depth:], -lhs[:depth]], 0)
        both = jnp.concatenate([lhs, crossed], 1)
        rhs = ext[:, pl.ds(start, width)]
        rows = lax.dot_general(both, rhs, (((0,), (0,)), ((), ())), preferred_element_type=jnp.float32)
        for sub in range(q):
            part[first + sub, :, 0:width] = rows[sub * own : (sub + 1) * own]
            part[first + sub, :, width : 2 * width] = rows[block + sub * own : block + (sub + 1) * own]
        return 0

    lax.fori_loop(0, blocks, compute, 0)

    def gather_in(v, upto):
        where = place(flips_of(v))
        names = [name(flips_of(v | (1 << (nbits - 1 - t)))) for t in range(upto)]
        for ident in names:
            message(where, ident, partner[0]).wait_recv()
        for r in range(0, own, 8):
            rows = pl.ds(r, 8)
            total = part[where, rows, :]
            for ident in names:
                total = total + land[ident, rows, :]
            part[where, rows, :] = total
        return where

    for s in range(1, nbits):
        top = 1 << (nbits - 1 - s)
        for w in range(top - 1, -1, -1):
            v = top + w
            where = gather_in(v, s)
            message(where, name(flips_of(v)), partner[s]).start()

    gather_in(0, nbits)
    for r in range(0, own, 8):
        rows = pl.ds(r, 8)
        kept[rows, :] = part[me, rows, :] / total_cols

    mine = me // q
    sub_me = me % q

    def mirror(k, sub):
        target = ((mine + k) % blocks) * q + sub
        return pltpu.make_async_remote_copy(
            src_ref=turned.at[k - 1, pl.ds(sub * own, own)],
            dst_ref=came.at[(k - 1) * q + sub_me],
            send_sem=msend.at[(k - 1) * q + sub],
            recv_sem=mrecv.at[(k - 1) * q + sub_me],
            device_id=coords(target, sizes),
            device_id_type=MESH,
        )

    for k in range(1, blocks // 2):
        cols = kept[:, k * block : (k + 1) * block]
        more = kept[:, width + k * block : width + (k + 1) * block]
        turned[k - 1] = jnp.concatenate([cols, more], 0).T
    for k in range(1, blocks // 2):
        for sub in range(q):
            mirror(k, sub).start()
    for k in range(1, blocks // 2):
        for sub in range(q):
            slot = (k - 1) * q + sub
            pltpu.make_async_remote_copy(
                src_ref=turned.at[k - 1, pl.ds(sub * own, own)],
                dst_ref=came.at[slot],
                send_sem=msend.at[slot],
                recv_sem=mrecv.at[slot],
                device_id=coords(((mine + k) % blocks) * q + sub, sizes),
                device_id_type=MESH,
            ).wait()
            mirrored[slot] = came[slot]

    def drain(ident, _):
        message(0, ident, partner[0]).wait_send()
        return 0

    lax.fori_loop(1, n, drain, 0)


def finish_kernel(sizes, kept, mirrored, px, pz, phase, real, imag, expect):
    n = sizes[0] * sizes[1] * sizes[2]
    own, order = real.shape
    block = max(own, LANES)
    q = block // own
    blocks = order // block
    width = (blocks // 2 + 1) * block
    me = flat_index(sizes)
    mine = me // q

    def columns(k):
        return pl.ds(pl.multiple_of(((mine + k + blocks) % blocks) * block, block), block)

    for k in range(blocks // 2 + 1):
        real[:, columns(k)] = kept[:, k * block : (k + 1) * block]
        imag[:, columns(k)] = kept[:, width + k * block : width + (k + 1) * block]
    for k in range(1, blocks // 2):
        tiles = [mirrored[(k - 1) * q + sub] for sub in range(q)]
        real[:, columns(-k)] = jnp.concatenate([t[:, :own] for t in tiles], 1)
        imag[:, columns(-k)] = -jnp.concatenate([t[:, own:] for t in tiles], 1)

    terms = px.shape[0]
    base = me * own
    ids = base + lax.broadcasted_iota(jnp.int32, (terms, own), 1)
    anded = jnp.bitwise_and(ids, pz[...])
    shift = 16
    while shift >= 1:
        anded = jnp.bitwise_xor(anded, jnp.right_shift(anded, shift))
        shift //= 2
    signs = (1 - 2 * jnp.bitwise_and(anded, 1)).astype(jnp.float32)
    wanted = jnp.bitwise_xor(px[...], base)
    row = lax.broadcasted_iota(jnp.int32, (own, block), 0)
    lane = lax.broadcasted_iota(jnp.int32, (own, block), 1)
    lane_terms = lax.broadcasted_iota(jnp.int32, (terms, block), 1)

    def picked(ref, tile):
        values = ref[:, pl.ds(pl.multiple_of(tile * block, block), block)]
        for p in range(log2(own)):
            step = 1 << p
            swapped = jnp.where(
                jnp.bitwise_and(lane, step) != 0,
                pltpu.roll(values, step, 1),
                pltpu.roll(values, block - step, 1),
            )
            values = jnp.where(jnp.bitwise_and(row, step) != 0, swapped, values)
        sums = lax.dot_general(
            signs, values, (((1,), (0,)), ((), ())), precision=lax.Precision.HIGHEST, preferred_element_type=jnp.float32
        )
        return jnp.where(lane_terms + tile * block == wanted, sums, 0.0)

    def body(tile, carry):
        return carry[0] + picked(real, tile), carry[1] + picked(imag, tile)

    zeros = jnp.zeros((terms, block), jnp.float32)
    sum_real, sum_imag = lax.fori_loop(0, blocks, body, (zeros, zeros))
    sum_real = jnp.sum(sum_real, axis=1, keepdims=True)
    sum_imag = jnp.sum(sum_imag, axis=1, keepdims=True)
    turn = phase[...]
    phase_real = jnp.where(turn == 0, 1.0, jnp.where(turn == 2, -1.0, 0.0))
    phase_imag = jnp.where(turn == 1, 1.0, jnp.where(turn == 3, -1.0, 0.0))
    expect[:, 0:1] = phase_real * sum_real - phase_imag * sum_imag
    expect[:, 1:2] = phase_real * sum_imag + phase_imag * sum_real


def on_device(sizes, amplitudes, pauli_x, pauli_z, pauli_phase):
    n = sizes[0] * sizes[1] * sizes[2]
    _, depth, order = amplitudes.shape
    own = order // n
    block = max(own, LANES)
    q = block // own
    blocks = order // block
    width = (blocks // 2 + 1) * block
    slots = (blocks // 2 - 1) * q
    vmem = pl.BlockSpec(memory_space=pltpu.VMEM)
    kept, mirrored = pl.pallas_call(
        functools.partial(gram_kernel, sizes, float(depth * n)),
        out_shape=(
            jax.ShapeDtypeStruct((own, 2 * width), jnp.float32),
            jax.ShapeDtypeStruct((slots, own, 2 * own), jnp.float32),
        ),
        in_specs=[pl.BlockSpec(memory_space=pl.ANY)],
        out_specs=(vmem, vmem),
        scratch_shapes=[
            pltpu.VMEM((2 * depth, order + width - block), jnp.bfloat16),
            pltpu.VMEM((n, own, 2 * width), jnp.float32),
            pltpu.VMEM((n, own, 2 * width), jnp.float32),
            pltpu.VMEM((blocks // 2 - 1, block, 2 * own), jnp.float32),
            pltpu.VMEM((slots, own, 2 * own), jnp.float32),
            pltpu.SemaphoreType.DMA((4,)),
            pltpu.SemaphoreType.DMA((n,)),
            pltpu.SemaphoreType.DMA((n,)),
            pltpu.SemaphoreType.DMA((slots,)),
            pltpu.SemaphoreType.DMA((slots,)),
        ],
        compiler_params=pltpu.CompilerParams(has_side_effects=True, vmem_limit_bytes=60 << 20),
    )(amplitudes)
    terms = pauli_x.shape[0]
    real, imag, expect = pl.pallas_call(
        functools.partial(finish_kernel, sizes),
        out_shape=(
            jax.ShapeDtypeStruct((own, order), jnp.float32),
            jax.ShapeDtypeStruct((own, order), jnp.float32),
            jax.ShapeDtypeStruct((terms, 2), jnp.float32),
        ),
        in_specs=[vmem] * 5,
        out_specs=(vmem,) * 3,
    )(kept, mirrored, pauli_x[:, None], pauli_z[:, None], pauli_phase[:, None])
    return real, imag, lax.psum(expect.T, AXES)


def solution(mesh):
    sizes = tuple(mesh.shape[axis] for axis in AXES)
    return jax.shard_map(
        functools.partial(on_device, sizes),
        mesh=mesh,
        in_specs=(P(None, AXES, None), P(), P(), P()),
        out_specs=(P(AXES, None), P(AXES, None), P()),
        check_vma=False,
    )
```

```python
import functools

import jax
import jax.numpy as jnp
from jax import lax
from jax.experimental import pallas as pl
from jax.experimental.pallas import tpu as pltpu
from jax.sharding import PartitionSpec as P

AXES = ("gx", "gy", "gz")
LANES = 128
MESH = pl.DeviceIdType.MESH


def log2(value):
    return value.bit_length() - 1


def flat_index(sizes):
    return (lax.axis_index("gx") * sizes[1] + lax.axis_index("gy")) * sizes[2] + lax.axis_index("gz")


def coords(flat, sizes):
    return (flat // (sizes[1] * sizes[2]), (flat // sizes[2]) % sizes[1], flat % sizes[2])


def flip(bit, by):
    return bit + by - 2 * bit * by


def stage_order(sizes):
    zs = log2(sizes[2])
    ys = log2(sizes[1])
    xs = log2(sizes[0])
    rest_x = [zs + ys + t for t in range(xs - 1, 0, -1)]
    rest_y = [zs + t for t in range(ys)]
    rest_z = list(range(zs - 1, -1, -1))
    order = [zs + ys] + rest_x + rest_y[:1] + rest_z + rest_y[1:]
    trade = order.index(rest_z[0]) if rest_x and rest_z else 1
    return order, trade


def parity_sign(masked):
    shift = 16
    while shift >= 1:
        masked = jnp.bitwise_xor(masked, jnp.right_shift(masked, shift))
        shift //= 2
    return (1 - 2 * jnp.bitwise_and(masked, 1)).astype(jnp.float32)


def gram_kernel(
    sizes, total_cols, amp, px, pz, phase, kept, mirrored, expect,
    ext, part, land, turned, came, outbox, inbox, load_sem, send_sem, recv_sem, msend, mrecv, esend, erecv,
):
    n = sizes[0] * sizes[1] * sizes[2]
    nbits = log2(n)
    depth = amp.shape[1]
    order = amp.shape[2]
    own = order // n
    block = max(own, LANES)
    q = block // own
    blocks = order // block
    width = (blocks // 2 + 1) * block
    me = flat_index(sizes)
    bits = [(me // (1 << p)) % 2 for p in range(nbits)]
    stages, trade = stage_order(sizes)
    half = bits[stages[0]]

    def loads():
        out = []
        for part_index in range(2):
            rows = pl.ds(part_index * depth, depth)
            out.append(pltpu.make_async_copy(amp.at[part_index], ext.at[rows, pl.ds(0, order)], load_sem.at[2 * part_index]))
            out.append(
                pltpu.make_async_copy(
                    amp.at[part_index, :, pl.ds(0, width - block)],
                    ext.at[rows, pl.ds(order, width - block)],
                    load_sem.at[2 * part_index + 1],
                )
            )
        return out

    for copy in loads():
        copy.start()

    def flips_of(v):
        by_stage = [(v >> (nbits - 1 - s)) & 1 for s in range(nbits)]
        flips = [0] * nbits
        for s, p in enumerate(stages):
            flips[p] = by_stage[s]
        if by_stage[1] != by_stage[trade]:
            flips[stages[1]] = by_stage[1] * (1 - half) + by_stage[trade] * half
            flips[stages[trade]] = by_stage[trade] * (1 - half) + by_stage[1] * half
        return flips

    def place(flips):
        return sum((1 << p) * flip(bits[p], flips[p]) for p in range(nbits))

    def name(flips):
        return sum((1 << p) * flips[p] for p in range(nbits))

    def message(where, ident, target):
        return pltpu.make_async_remote_copy(
            src_ref=part.at[where],
            dst_ref=land.at[ident],
            send_sem=send_sem.at[ident],
            recv_sem=recv_sem.at[ident],
            device_id=coords(target, sizes),
            device_id_type=MESH,
        )

    partner = [place(flips_of(1 << (nbits - 1 - s))) for s in range(nbits)]
    lowbits = log2(q)
    high = [p for p in stages[-1:] + stages[1:-1] if p >= lowbits]

    def row_block(u):
        flips = [0] * nbits
        flips[stages[0]] = 1 - u % 2
        for j, p in enumerate(high):
            flips[p] = 1 - (u // (1 << (len(high) - j))) % 2
        return flips

    for copy in loads():
        copy.wait()

    def add_in(where, names):
        for ident in names:
            message(where, ident, partner[0]).wait_recv()
        for r in range(0, own, 8):
            rows = pl.ds(r, 8)
            total = part[where, rows, :]
            for ident in names:
                total = total + land[ident, rows, :]
            part[where, rows, :] = total

    def with_low(flips, g):
        return [(g >> p) & 1 if p < lowbits else flips[p] for p in range(nbits)]

    def second_stage(w):
        for g in range(q):
            flips = with_low(row_block(2 * w + 1), g)
            goes = flips[stages[1]] * (1 - half) + flips[stages[trade]] * half

            @pl.when(goes == 1)
            def _():
                where, ident = place(flips), name(flips)
                add_in(where, [ident + (1 << stages[0])])
                message(where, ident, partner[1]).start()

    def compute(u, _):
        @pl.when(u % 2 == 1)
        def _():
            for g in range(q):
                flips = with_low(row_block(u - 1), g)
                message(place(flips), name(flips), partner[0]).start()

        @pl.when((u % 2 == 1) & (u >= 5))
        def _():
            second_stage(u // 2 - 2)

        flips = row_block(u)
        first = sum((1 << p) * flip(bits[p], flips[p]) for p in range(lowbits, nbits))
        start = pl.multiple_of(first * own, block)
        lhs = ext[:, pl.ds(start, block)]
        crossed = jnp.concatenate([lhs[depth:], -lhs[:depth]], 0)
        both = jnp.concatenate([lhs, crossed], 1)
        rhs = ext[:, pl.ds(start, width)]
        rows = lax.dot_general(both, rhs, (((0,), (0,)), ((), ())), preferred_element_type=jnp.float32)
        for sub in range(q):
            part[first + sub, :, 0:width] = rows[sub * own : (sub + 1) * own]
            part[first + sub, :, width : 2 * width] = rows[block + sub * own : block + (sub + 1) * own]
        return 0

    lax.fori_loop(0, blocks, compute, 0)

    for w in range(max(blocks // 2 - 2, 0), blocks // 2):
        second_stage(w)

    def gather_in(v, upto):
        where = place(flips_of(v))
        add_in(where, [name(flips_of(v | (1 << (nbits - 1 - t)))) for t in range(upto)])
        return where

    later = 1 << (nbits - 2)
    for v in sorted(range(1, later), key=lambda v: (v % 2 == 0, -v)):
        s = nbits - v.bit_length()
        where = gather_in(v, s)
        message(where, name(flips_of(v)), partner[s]).start()

    gather_in(0, nbits)
    for r in range(0, own, 8):
        rows = pl.ds(r, 8)
        kept[rows, :] = part[me, rows, :] / total_cols

    mine = me // q
    sub_me = me % q

    def mirror(k, sub):
        target = ((mine + k) % blocks) * q + sub
        return pltpu.make_async_remote_copy(
            src_ref=turned.at[k - 1, pl.ds(sub * own, own)],
            dst_ref=came.at[(k - 1) * q + sub_me],
            send_sem=msend.at[(k - 1) * q + sub],
            recv_sem=mrecv.at[(k - 1) * q + sub_me],
            device_id=coords(target, sizes),
            device_id_type=MESH,
        )

    for k in range(1, blocks // 2):
        cols = kept[:, k * block : (k + 1) * block]
        more = kept[:, width + k * block : width + (k + 1) * block]
        turned[k - 1] = jnp.concatenate([cols, more], 0).T
    for k in range(1, blocks // 2):
        for sub in range(q):
            mirror(k, sub).start()
    terms = px.shape[1]
    base = me * own
    ids = base + lax.broadcasted_iota(jnp.int32, (own, terms), 0)
    signs = parity_sign(jnp.bitwise_and(ids, pz[...]))
    paired = parity_sign(jnp.bitwise_and(px[...], pz[...]))
    wanted = jnp.bitwise_xor(px[...], base)
    row = lax.broadcasted_iota(jnp.int32, (own, block), 0)
    lane = lax.broadcasted_iota(jnp.int32, (own, block), 1)
    lane_terms = lax.broadcasted_iota(jnp.int32, (block, terms), 0)

    def picked(first, k):
        values = kept[:, first + k * block : first + (k + 1) * block]
        for p in range(log2(own)):
            step = 1 << p
            swapped = jnp.where(
                jnp.bitwise_and(lane, step) != 0,
                pltpu.roll(values, step, 1),
                pltpu.roll(values, block - step, 1),
            )
            values = jnp.where(jnp.bitwise_and(row, step) != 0, swapped, values)
        sums = lax.dot_general(
            values, signs, (((0,), (0,)), ((), ())), precision=lax.Precision.HIGHEST, preferred_element_type=jnp.float32
        )
        chosen = jnp.where(lane_terms + ((mine + k) % blocks) * block == wanted, sums, 0.0)
        return jnp.sum(chosen, axis=0, keepdims=True)

    def row_sums(first, sign):
        ends = picked(first, 0) + picked(first, blocks // 2)
        inner = jnp.zeros_like(ends)
        for k in range(1, blocks // 2):
            inner = inner + picked(first, k)
        return ends + inner * (1.0 + sign * paired)

    sum_real = row_sums(0, 1.0)
    sum_imag = row_sums(width, -1.0)
    turn = phase[...]
    phase_real = jnp.where(turn == 0, 1.0, jnp.where(turn == 2, -1.0, 0.0))
    phase_imag = jnp.where(turn == 1, 1.0, jnp.where(turn == 3, -1.0, 0.0))
    total = jnp.concatenate(
        [phase_real * sum_real - phase_imag * sum_imag, phase_real * sum_imag + phase_imag * sum_real], 0
    )
    here = coords(me, sizes)
    first_slot = 0
    for axis in range(3):
        size = sizes[axis]
        at = here[axis]
        outbox[axis] = total
        inbox[first_slot + at] = total
        copies = []
        for d in range(1, size):
            target = list(here)
            target[axis] = (at + d) % size
            copies.append(
                pltpu.make_async_remote_copy(
                    src_ref=outbox.at[axis],
                    dst_ref=inbox.at[first_slot + at],
                    send_sem=esend.at[first_slot + d],
                    recv_sem=erecv.at[first_slot + at],
                    device_id=tuple(target),
                    device_id_type=MESH,
                )
            )
        for copy in copies:
            copy.start()
        for d in range(1, size):
            source = first_slot + (at + d) % size
            pltpu.make_async_remote_copy(
                src_ref=outbox.at[axis],
                dst_ref=inbox.at[source],
                send_sem=esend.at[first_slot + d],
                recv_sem=erecv.at[source],
                device_id=tuple(target),
                device_id_type=MESH,
            ).wait()
        total = inbox[first_slot]
        for j in range(1, size):
            total = total + inbox[first_slot + j]
        first_slot += size
    expect[...] = total

    for k in range(1, blocks // 2):
        for sub in range(q):
            slot = (k - 1) * q + sub
            pltpu.make_async_remote_copy(
                src_ref=turned.at[k - 1, pl.ds(sub * own, own)],
                dst_ref=came.at[slot],
                send_sem=msend.at[slot],
                recv_sem=mrecv.at[slot],
                device_id=coords(((mine + k) % blocks) * q + sub, sizes),
                device_id_type=MESH,
            ).wait()
            mirrored[slot] = came[slot]

    def drain(ident, _):
        message(0, ident, partner[0]).wait_send()
        return 0

    lax.fori_loop(1, n, drain, 0)


def finish_kernel(sizes, kept, mirrored, real, imag):
    n = sizes[0] * sizes[1] * sizes[2]
    own, order = real.shape
    block = max(own, LANES)
    q = block // own
    blocks = order // block
    width = (blocks // 2 + 1) * block
    me = flat_index(sizes)
    mine = me // q

    def columns(k):
        return pl.ds(pl.multiple_of(((mine + k + blocks) % blocks) * block, block), block)

    for k in range(blocks // 2 + 1):
        real[:, columns(k)] = kept[:, k * block : (k + 1) * block]
        imag[:, columns(k)] = kept[:, width + k * block : width + (k + 1) * block]
    for k in range(1, blocks // 2):
        tiles = [mirrored[(k - 1) * q + sub] for sub in range(q)]
        real[:, columns(-k)] = jnp.concatenate([t[:, :own] for t in tiles], 1)
        imag[:, columns(-k)] = -jnp.concatenate([t[:, own:] for t in tiles], 1)


def on_device(sizes, amplitudes, pauli_x, pauli_z, pauli_phase):
    n = sizes[0] * sizes[1] * sizes[2]
    _, depth, order = amplitudes.shape
    own = order // n
    block = max(own, LANES)
    q = block // own
    blocks = order // block
    width = (blocks // 2 + 1) * block
    slots = (blocks // 2 - 1) * q
    vmem = pl.BlockSpec(memory_space=pltpu.VMEM)
    terms = pauli_x.shape[0]
    kept, mirrored, expect = pl.pallas_call(
        functools.partial(gram_kernel, sizes, float(depth * n)),
        out_shape=(
            jax.ShapeDtypeStruct((own, 2 * width), jnp.float32),
            jax.ShapeDtypeStruct((slots, own, 2 * own), jnp.float32),
            jax.ShapeDtypeStruct((2, terms), jnp.float32),
        ),
        in_specs=[pl.BlockSpec(memory_space=pl.ANY), vmem, vmem, vmem],
        out_specs=(vmem,) * 3,
        scratch_shapes=[
            pltpu.VMEM((2 * depth, order + width - block), jnp.bfloat16),
            pltpu.VMEM((n, own, 2 * width), jnp.float32),
            pltpu.VMEM((n, own, 2 * width), jnp.float32),
            pltpu.VMEM((blocks // 2 - 1, block, 2 * own), jnp.float32),
            pltpu.VMEM((slots, own, 2 * own), jnp.float32),
            pltpu.VMEM((3, 2, terms), jnp.float32),
            pltpu.VMEM((sum(sizes), 2, terms), jnp.float32),
            pltpu.SemaphoreType.DMA((4,)),
            pltpu.SemaphoreType.DMA((n,)),
            pltpu.SemaphoreType.DMA((n,)),
            pltpu.SemaphoreType.DMA((slots,)),
            pltpu.SemaphoreType.DMA((slots,)),
            pltpu.SemaphoreType.DMA((sum(sizes),)),
            pltpu.SemaphoreType.DMA((sum(sizes),)),
        ],
        compiler_params=pltpu.CompilerParams(has_side_effects=True, vmem_limit_bytes=60 << 20),
    )(amplitudes, pauli_x[None], pauli_z[None], pauli_phase[None])
    real, imag = pl.pallas_call(
        functools.partial(finish_kernel, sizes),
        out_shape=(
            jax.ShapeDtypeStruct((own, order), jnp.float32),
            jax.ShapeDtypeStruct((own, order), jnp.float32),
        ),
        in_specs=[vmem] * 2,
        out_specs=(vmem,) * 2,
    )(kept, mirrored)
    return real, imag, expect


def solution(mesh):
    sizes = tuple(mesh.shape[axis] for axis in AXES)
    return jax.shard_map(
        functools.partial(on_device, sizes),
        mesh=mesh,
        in_specs=(P(None, AXES, None), P(), P(), P()),
        out_specs=(P(AXES, None), P(AXES, None), P()),
        check_vma=False,
    )
```
